32 devices in a mesh: rep: 1 (over z), dp: 32 (over x, y, core).
Axes of the slice: x: 4, y: 4, z: 1, core: 2. Of those that a mesh axis runs over, the one named last changes fastest.
The devices are a block of a 4x4x8 slice.
Arguments:
- g_w_gate: bfloat16 [32, 2, 1024, 3328], P(('rep', 'dp'))
- g_w_up: bfloat16 [32, 2, 1024, 3328], P(('rep', 'dp'))
- g_w_down: bfloat16 [32, 2, 3328, 1024], P(('rep', 'dp'))
- w_gate: bfloat16 [2, 1024, 3328], replicated
- w_up: bfloat16 [2, 1024, 3328], replicated
- w_down: bfloat16 [2, 3328, 1024], replicated
- m_w_gate: float32 [2, 1024, 3328], P(None, 'dp')
- m_w_up: float32 [2, 1024, 3328], P(None, 'dp')
- m_w_down: float32 [2, 3328, 1024], P(None, 'dp')
- v_w_gate: float32 [2, 1024, 3328], P(None, 'dp')
- v_w_up: float32 [2, 1024, 3328], P(None, 'dp')
- v_w_down: float32 [2, 3328, 1024], P(None, 'dp')
Outputs:
- output 1: bfloat16 [2, 1024, 3328], P('rep')
- output 2: bfloat16 [2, 1024, 3328], P('rep')
- output 3: bfloat16 [2, 3328, 1024], P('rep')
- output 4: float32 [2, 1024, 3328], P('rep', 'dp')
- output 5: float32 [2, 1024, 3328], P('rep', 'dp')
- output 6: float32 [2, 3328, 1024], P('rep', 'dp')
- output 7: float32 [2, 1024, 3328], P('rep', 'dp')
- output 8: float32 [2, 1024, 3328], P('rep', 'dp')
- output 9: float32 [2, 3328, 1024], P('rep', 'dp')
All inputs are finite; a program needn't handle non-finite values.
Results may differ from the reference program's by a relative error of at most 0.022.
Values are sent between devices in bfloat16 or wider.
A program may use at most 768 MiB of HBM per device.

```python
import jax
import jax.numpy as jnp
from jax import lax

DEVICES = 32
D = 1024
FF = 3328
LAYERS = 2
NAMES = ("w_gate", "w_up", "w_down")
SHAPES = {"w_gate": (LAYERS, D, FF), "w_up": (LAYERS, D, FF), "w_down": (LAYERS, FF, D)}


def setup_inputs(seed: int = 0, part: int = 0) -> dict:
    kz, *keys = jax.random.split(jax.random.key(seed), 1 + 5 * len(NAMES))
    loud = 2.0 ** jax.random.uniform(kz, (), jnp.float32, -1.0, 1.0)
    drawn = {}
    for name, key, both in zip(NAMES, keys[:3], keys[3:6], strict=True):
        own = jax.random.normal(jax.random.fold_in(key, part), (DEVICES, *SHAPES[name]), jnp.float32)
        shared = jax.random.normal(jax.random.fold_in(both, part), SHAPES[name], jnp.float32)
        drawn["g_" + name] = (loud * (0.7 * shared / DEVICES + 0.7 * own * DEVICES**-0.5)).astype(jnp.bfloat16)
    for name, key in zip(NAMES, keys[6:9], strict=True):
        drawn[name] = (jax.random.normal(key, SHAPES[name], jnp.float32) * SHAPES[name][1] ** -0.5).astype(jnp.bfloat16)
    for name, key in zip(NAMES, keys[9:12], strict=True):
        drawn["m_" + name] = loud * 0.5 * jax.random.normal(key, SHAPES[name], jnp.float32)
    for name, key in zip(NAMES, keys[12:15], strict=True):
        drawn["v_" + name] = loud * loud * jax.random.uniform(key, SHAPES[name], jnp.float32, 0.5, 1.5)
    return drawn


def adamw(w, m, v, g):
    m = 0.9 * m + 0.1 * g
    v = 0.95 * v + 0.05 * g * g
    step = m * lax.rsqrt(v + 1e-8) + 0.1 * w
    return (w - 0.02 * step).astype(jnp.bfloat16), m, v


def reference(g_w_gate, g_w_up, g_w_down, w_gate, w_up, w_down, m_w_gate, m_w_up, m_w_down, v_w_gate, v_w_up, v_w_down):
    def total(terms):
        return lax.scan(lambda so_far, term: (so_far + term.astype(jnp.float32), None), jnp.zeros(terms.shape[1:], jnp.float32), terms)[0]

    gradients = [total(terms).astype(jnp.bfloat16).astype(jnp.float32) for terms in (g_w_gate, g_w_up, g_w_down)]
    new = [
        adamw(w.astype(jnp.float32), m, v, g)
        for w, m, v, g in zip((w_gate, w_up, w_down), (m_w_gate, m_w_up, m_w_down), (v_w_gate, v_w_up, v_w_down), gradients, strict=True)
    ]
    return tuple(one[which] for which in range(3) for one in new)
```

```python
import functools
import math

import jax
import jax.numpy as jnp
from jax import lax
from jax.experimental import pallas as pl
from jax.experimental.pallas import tpu as pltpu
from jax.sharding import PartitionSpec as P

F32, BF16 = jnp.float32, jnp.bfloat16
RING = 4
CORES = 2
PER_MATRIX = 2
VMEM_LIMIT = 17050 << 10
EARLY_SLOTS = 2
SLOTS = 3

TURN = {'send_half': (-17.7, 10.6), 'load_half': (-8.4, 10.6), 'load_other': (-8.0, 10.6), 'rs1': (-3.6, 10.6), 'rs1_relay_load': (3.5, 10.6), 'rs1_relay': (5.0, 10.6), 'rs2_load': (12.4, 10.6), 'rs2': (13.3, 10.6), 'rs2_relay': (17.1, 10.6), 'update': (21.6, 10.6), 'ag1_own': (24.0, 12.24), 'ag2_relay': (24.8, 12.24), 'ag1_near': (25.3, 12.24), 'ag1_far': (31.0, 12.24), 'ag1_relay': (44.8, 12.24), 'ag1_relay_far': (48.3, 12.24), 'last': (66.1, 12.24)}


def as_tiles(a, rows):
    *lead, r, c = a.shape
    n = len(lead)
    a = a.reshape(*lead, r // 8, 8, c // 128, 128).transpose(*range(n), n, n + 2, n + 1, n + 3)
    return a.reshape(*lead, r // rows, rows // 8 * (c // 128), 8, 128)


def from_tiles(a, rows, columns):
    lead = a.shape[: a.ndim - 4]
    n = len(lead)
    a = a.reshape(*lead, rows // 8, columns // 128, 8, 128).transpose(*range(n), n, n + 2, n + 1, n + 3)
    return a.reshape(*lead, rows, columns)


def kernel(chunks, *refs):
    g_refs, w_refs, m_refs, v_refs = (refs[i : i + 3] for i in (0, 3, 6, 9))
    out_refs, mo_refs, vo_refs = (refs[i : i + 3] for i in (12, 15, 18))
    half_ref, line_ref = refs[21:23]
    own, early, late, s1, s2, recv, sent, near = refs[23:]

    me = lax.axis_index("dp")
    core, chip = me % CORES, me // CORES
    x, y = chip // RING, chip % RING
    mate = 1 - core

    def place(ra, rb):
        return (x + ra * mate + rb * core) % RING * RING + (y + rb * mate + ra * core) % RING

    chips = [[place(ra, rb) for rb in range(RING)] for ra in range(RING)]
    right, left = chips[1][0] * CORES + core, chips[RING - 1][0] * CORES + core
    up, down = chips[0][1] * CORES + core, chips[0][RING - 1] * CORES + core
    partner = chip * CORES + mate

    barrier = pltpu.get_barrier_semaphore()
    peers = (right, left, up, down, partner)
    for peer in peers:
        pl.semaphore_signal(barrier, inc=1, device_id={"dp": peer}, device_id_type=pl.DeviceIdType.MESH)
    pl.semaphore_wait(barrier, len(peers))

    def copy_to(device, src, dst, send_sem, recv_sem):
        pltpu.make_async_remote_copy(
            src_ref=src, dst_ref=dst, send_sem=send_sem, recv_sem=recv_sem, device_id={"dp": device}, device_id_type=pl.DeviceIdType.MESH
        ).start()

    def wait(ref, sem):
        pltpu.make_async_copy(ref, ref, sem).wait()

    kinds = (
        "half", "relay_l", "relay_r", "fl_direct", "fl_relay", "fr_direct", "fr_relay", "relay_d",
        "relay_u", "fd_direct", "fd_relay", "fu_direct", "fu_relay", "g2_d", "g2_u", "g2_far_d",
        "g2_far_u", "g1_l0", "g1_l1", "g1_l2", "g1_l3", "g1_r0", "g1_r1", "g1_r2",
        "g1_r3", "far_0", "far_3", "far_1l", "far_1r", "far_2l", "far_2r", "core",
    )

    def rsem(k, kind):
        return recv.at[k, kinds.index(kind)]

    def total(dst, at, sources, tiles, unroll):
        @pl.loop(0, tiles // unroll)
        def _(i):
            parts = [ref[pl.ds(start + i * unroll, unroll)].astype(F32) for ref, start in sources]
            dst[pl.ds(at + i * unroll, unroll)] = functools.reduce(jnp.add, parts).astype(BF16)

    class Chunk:
        pass

    cs = []
    base = 0
    for k, (weight, layer, t0, nt) in enumerate(chunks):
        c = Chunk()
        c.k, c.weight, c.layer, c.t0, c.nt, c.h, c.base = k, weight, layer, t0, nt, nt // 2, base
        c.own, c.s1, c.s2 = own.at[k % SLOTS], s1.at[k % SLOTS], s2.at[k]
        c.early, c.late = early.at[k % EARLY_SLOTS], late.at[k % SLOTS]
        c.landing = line_ref.at[pl.ds(base // (RING * RING) * 12, 12 * nt)]
        base += RING * RING * nt
        cs.append(c)

    def out_at(c, where, which, t=0, n=None):
        return out_refs[c.weight].at[c.layer, where, which, pl.ds(c.t0 + t, c.nt if n is None else n)]

    def spread(c, where, device, kind, t=0, n=None):
        piece = out_at(c, where, core, t, n)
        copy_to(device, piece, piece, sent.at[c.k, 1], rsem(c.k, kind))

    def send_half(c):
        @pl.loop(0, RING * RING)
        def _(i):
            src = g_refs[c.weight].at[c.layer, place(i % RING, i // RING), mate, pl.ds(c.t0, c.nt)]
            copy_to(partner, src, half_ref.at[pl.ds(c.base + i * c.nt, c.nt)], sent.at[c.k, 1], rsem(c.k, "half"))

    def load_half(c):
        if c.k >= SLOTS:
            old = cs[c.k - SLOTS]
            n = 14 * old.nt
            wait(half_ref.at[pl.ds(0, n)], sent.at[old.k, 0])

        @pl.loop(0, RING * RING)
        def _(i):
            src = g_refs[c.weight].at[c.layer, place(i // RING, i % RING), core, pl.ds(c.t0, c.nt)]
            pltpu.make_async_copy(src, c.own.at[pl.ds(i * c.nt, c.nt)], near.at[c.k, 0]).start()

    def other(c, piece):
        if 6 <= piece < 14:
            return c.early, (piece - 6) * c.nt
        return c.late, (piece if piece < 6 else piece - 8) * c.nt

    def load_other(c):
        nt = c.nt
        wait(half_ref.at[pl.ds(c.base, RING * RING * nt)], rsem(c.k, "half"))
        for i, (dst, to, piece, n) in enumerate(((c.early, 0, 6, 8), (c.late, 0, 0, 6), (c.late, 6, 14, 2))):
            src = half_ref.at[pl.ds(c.base + piece * nt, n * nt)]
            pltpu.make_async_copy(src, dst.at[pl.ds(to * nt, n * nt)], near.at[c.k, (1, 7, 8)[i]]).start()

    def rs1(c):
        nt, n = c.nt, RING * RING * c.nt
        wait(c.own.at[pl.ds(0, n)], near.at[c.k, 0])
        wait(c.early.at[pl.ds(0, 8 * nt)], near.at[c.k, 1])
        for piece, device, at, kind in ((8, right, 0, "relay_l"), (10, left, 2, "relay_r"), (6, right, 6, "fl_direct"), (12, left, 8, "fr_direct")):
            total(c.own, piece * nt, [(c.own, piece * nt), other(c, piece)], 2 * nt, 13)
            copy_to(device, c.own.at[pl.ds(piece * nt, 2 * nt)], c.landing.at[pl.ds(at * nt, 2 * nt)], sent.at[c.k, 0], rsem(c.k, kind))

    def rs1_relay_load(c):
        n = 4 * c.nt
        for at, kind in ((0, "relay_l"), (2, "relay_r")):
            wait(c.landing.at[pl.ds(at * c.nt, 2 * c.nt)], rsem(c.k, kind))
        pltpu.make_async_copy(c.landing.at[pl.ds(0, n)], c.s1.at[pl.ds(0, n)], near.at[c.k, 2]).start()

    def rs1_relay(c):
        nt = c.nt
        wait(c.late.at[pl.ds(0, 6 * nt)], near.at[c.k, 7])
        wait(c.late.at[pl.ds(6 * nt, 2 * nt)], near.at[c.k, 8])
        wait(c.s1.at[pl.ds(0, 4 * nt)], near.at[c.k, 2])
        for piece, device, at, to, kind in ((4, right, 0, 4, "fl_relay"), (14, left, 2, 10, "fr_relay")):
            total(c.s1, at * nt, [(c.own, piece * nt), other(c, piece), (c.s1, at * nt)], 2 * nt, 13)
            copy_to(device, c.s1.at[pl.ds(at * nt, 2 * nt)], c.landing.at[pl.ds(to * nt, 2 * nt)], sent.at[c.k, 0], rsem(c.k, kind))

    def line(c, rb, t):
        nt = c.nt
        return [(c.own, rb * nt + t), (c.late, rb * nt + t), (c.s1, (4 + rb) * nt + t), (c.s1, (8 + rb) * nt + t)]

    def rs2_load(c):
        nt = c.nt
        for at, kind in ((4, "fl_relay"), (6, "fl_direct"), (8, "fr_direct"), (10, "fr_relay")):
            wait(c.landing.at[pl.ds(at * nt, 2 * nt)], rsem(c.k, kind))
        pltpu.make_async_copy(c.landing.at[pl.ds(4 * nt, 8 * nt)], c.s1.at[pl.ds(4 * nt, 8 * nt)], near.at[c.k, 6]).start()

    def rs2(c):
        nt, h = c.nt, c.h
        wait(c.s1.at[pl.ds(4 * nt, 8 * nt)], near.at[c.k, 6])
        for rb, t, n, device, to, kind in (
            (2, 0, h, up, 0, "relay_d"),
            (2, h, nt - h, down, h, "relay_u"),
            (1, h, nt - h, up, nt + h, "fd_direct"),
            (3, 0, h, down, 2 * nt, "fu_direct"),
        ):
            total(c.own, rb * nt + t, line(c, rb, t), n, 13)
            copy_to(device, c.own.at[pl.ds(rb * nt + t, n)], c.s2.at[pl.ds(to, n)], sent.at[c.k, 0], rsem(c.k, kind))

    def rs2_relay(c):
        nt, h = c.nt, c.h
        for rb, t, n, device, to, kind, kind_to in ((1, 0, h, up, nt, "relay_d", "fd_relay"), (3, h, nt - h, down, 2 * nt + h, "relay_u", "fu_relay")):
            here = c.s2.at[pl.ds(t, n)]
            wait(here, rsem(c.k, kind))
            total(c.s2, t, [*line(c, rb, t), (c.s2, t)], n, 13)
            copy_to(device, here, c.s2.at[pl.ds(to, n)], sent.at[c.k, 1], rsem(c.k, kind_to))

    loaded = set()

    def update(c):
        nt, h = c.nt, c.h
        if c.weight not in loaded:
            loaded.add(c.weight)
            for i, (store, src) in enumerate(state(c.weight)):
                wait(store, near.at[c.weight, 3 + i])
        for at, n, kind in ((nt, h, "fd_relay"), (nt + h, nt - h, "fd_direct"), (2 * nt, h, "fu_direct"), (2 * nt + h, nt - h, "fu_relay")):
            wait(c.s2.at[pl.ds(at, n)], rsem(c.k, kind))
        w_store = out_refs[c.weight].at[c.layer, chip, core]
        m_store, v_store = mo_refs[c.weight].at[c.layer], vo_refs[c.weight].at[c.layer]
        sources = [*line(c, 0, 0), (c.s2, nt), (c.s2, 2 * nt)]
        unroll = 4

        @pl.loop(0, nt // unroll)
        def _(i):
            g = functools.reduce(jnp.add, [ref[pl.ds(start + i * unroll, unroll)].astype(F32) for ref, start in sources])
            g = g.astype(BF16).astype(F32)
            here = pl.ds(c.t0 + i * unroll, unroll)
            w = w_store[here].astype(F32)
            m = 0.9 * m_store[here] + 0.1 * g
            v = 0.95 * v_store[here] + 0.05 * g * g
            step = m * lax.rsqrt(v + 1e-8) + 0.1 * w
            w_store[here] = (w - 0.02 * step).astype(BF16)
            m_store[here] = m
            v_store[here] = v

        spread(c, chip, up, "g2_d")
        spread(c, chip, down, "g2_u")

    def ag1_own(c):
        spread(c, chip, right, "g1_l0")
        spread(c, chip, left, "g1_r0")
        spread(c, chip, partner, "core")

    def arrived(c, where, kind, t=0, n=None):
        wait(out_at(c, where, core, t, n), rsem(c.k, kind))

    def ag2_relay(c):
        arrived(c, chips[0][3], "g2_d")
        spread(c, chips[0][3], up, "g2_far_d", 0, c.h)
        arrived(c, chips[0][1], "g2_u")
        spread(c, chips[0][1], down, "g2_far_u", c.h, c.nt - c.h)

    def ag1_near(c):
        for rb in (3, 1):
            spread(c, chips[0][rb], right, f"g1_l{rb}")
            spread(c, chips[0][rb], left, f"g1_r{rb}")
            spread(c, chips[0][rb], partner, "core")

    def ag1_far(c):
        arrived(c, chips[0][2], "g2_far_d", 0, c.h)
        arrived(c, chips[0][2], "g2_far_u", c.h, c.nt - c.h)
        spread(c, chips[0][2], right, "g1_l2")
        spread(c, chips[0][2], left, "g1_r2")
        spread(c, chips[0][2], partner, "core")

    def relay(c, rb):
        for ra, kind in ((3, f"g1_l{rb}"), (1, f"g1_r{rb}")):
            arrived(c, chips[ra][rb], kind)
        if rb == 0:
            spread(c, chips[3][0], right, "far_0")
        elif rb == 3:
            spread(c, chips[1][3], left, "far_3")
        else:
            spread(c, chips[3][rb], right, f"far_{rb}l", 0, c.h)
            spread(c, chips[1][rb], left, f"far_{rb}r", c.h, c.nt - c.h)
        for ra in (3, 1):
            spread(c, chips[ra][rb], partner, "core")

    def ag1_relay(c):
        for rb in (0, 3, 1):
            relay(c, rb)

    def ag1_relay_far(c):
        relay(c, 2)

    def last(c):
        arrived(c, chips[2][0], "far_0")
        arrived(c, chips[2][3], "far_3")
        for rb in (1, 2):
            arrived(c, chips[2][rb], f"far_{rb}l", 0, c.h)
            arrived(c, chips[2][rb], f"far_{rb}r", c.h, c.nt - c.h)
        for rb in range(RING):
            spread(c, chips[2][rb], partner, "core")

    def state(weight):
        mine = w_refs[weight].at[:, chip, core]
        return ((out_refs[weight].at[:, chip, core], mine), (mo_refs[weight], m_refs[weight]), (vo_refs[weight], v_refs[weight]))

    tasks = dict(
        send_half=send_half, load_half=load_half, load_other=load_other, rs1=rs1,
        rs1_relay_load=rs1_relay_load, rs1_relay=rs1_relay, rs2_load=rs2_load, rs2=rs2, rs2_relay=rs2_relay,
        update=update, ag1_own=ag1_own, ag2_relay=ag2_relay, ag1_near=ag1_near, ag1_far=ag1_far, ag1_relay=ag1_relay,
        ag1_relay_far=ag1_relay_far, last=last,
    )
    rank = {name: i for i, name in enumerate(tasks)}
    order = sorted(((TURN[name][0] + TURN[name][1] * c.k, rank[name], name, c) for name in tasks for c in cs), key=lambda one: one[:2])
    turn = {(name, c.k): i for i, (_, _, name, c) in enumerate(order)}
    for k in range(len(cs)):
        assert turn["load_half", k] < turn["load_other", k]
        assert k < SLOTS or turn["update", k - SLOTS] < turn["load_half", k]
        assert k < EARLY_SLOTS or turn["rs1", k - EARLY_SLOTS] < turn["load_other", k]
    state_at = 3
    for i, (_, _, name, c) in enumerate(order):
        if i == state_at:
            for weight in range(3):
                for j, (store, src) in enumerate(state(weight)):
                    pltpu.make_async_copy(src, store, near.at[weight, 3 + j]).start()
        tasks[name](c)

    for c in cs:
        here = pl.ds(c.t0, c.nt)
        wait(out_refs[c.weight].at[c.layer, :, mate, here], rsem(c.k, "core"))
        wait(half_ref.at[pl.ds(0, 48 * c.nt)], sent.at[c.k, 1])
        if c.k >= len(cs) - SLOTS:
            wait(half_ref.at[pl.ds(0, 14 * c.nt)], sent.at[c.k, 0])


def put(*refs):
    n = len(refs) // 2
    srcs, dsts, sem = refs[:n], refs[n : 2 * n], refs[2 * n]
    copies = []
    for src, dst in zip(srcs, dsts, strict=True):
        for layer in range(src.shape[0]):
            step = src.shape[1] // 4
            for part in range(4):
                here = pl.ds(part * step, step)
                copies.append(pltpu.make_async_copy(src.at[layer, here], dst.at[layer, here], sem.at[len(copies)]))
    for copy in copies:
        copy.start()
    for copy in copies:
        copy.wait()


def solution(mesh):
    group = mesh.shape["dp"]
    assert group == CORES * RING * RING and math.isqrt(group // CORES) == RING

    def step(*arrays):
        terms, weights, m, v = (arrays[i : i + 3] for i in (0, 3, 6, 9))
        layers = m[0].shape[0]
        shapes = [one.shape for one in m]
        blocks = [as_tiles(t[0], s[1]) for t, s in zip(terms, shapes, strict=True)]
        blocks += [as_tiles(w, s[1]) for w, s in zip(weights, shapes, strict=True)]
        tiles = blocks[0].shape[2]
        blocks = [b.reshape(layers, RING * RING, CORES, tiles, 8, 128) for b in blocks]
        moments = [as_tiles(one, one.shape[1]).reshape(layers, tiles, 8, 128) for one in (*m, *v)]
        nt = tiles // PER_MATRIX
        chunks = [(weight, layer, part * nt, nt) for weight in range(3) for layer in range(layers) for part in range(PER_MATRIX)]
        count = len(chunks)
        whole = pltpu.VMEM(blocks[0].shape, BF16)
        moment = pltpu.VMEM(moments[0].shape, F32)
        hbm, vmem = pl.BlockSpec(memory_space=pltpu.HBM), pl.BlockSpec(memory_space=pltpu.VMEM)
        pieces = RING * RING
        out = pl.pallas_call(
            functools.partial(kernel, chunks),
            out_shape=[whole] * 3
            + [moment] * 6
            + [jax.ShapeDtypeStruct((count * pieces * nt, 8, 128), BF16), jax.ShapeDtypeStruct((count * 12 * nt, 8, 128), BF16)],
            in_specs=[hbm] * 12,
            out_specs=[vmem] * 9 + [hbm] * 2,
            scratch_shapes=[
                pltpu.VMEM((SLOTS, pieces * nt, 8, 128), BF16),
                pltpu.VMEM((EARLY_SLOTS, 8 * nt, 8, 128), BF16),
                pltpu.VMEM((SLOTS, 8 * nt, 8, 128), BF16),
                pltpu.VMEM((SLOTS, 12 * nt, 8, 128), BF16),
                pltpu.VMEM((count, 3 * nt, 8, 128), BF16),
                pltpu.SemaphoreType.DMA((count, 32)),
                pltpu.SemaphoreType.DMA((count, 2)),
                pltpu.SemaphoreType.DMA((count, 9)),
            ],
            compiler_params=pltpu.CompilerParams(collective_id=0, has_side_effects=True, vmem_limit_bytes=VMEM_LIMIT),
        )(*blocks, *moments)[:9]
        out = [pltpu.with_memory_space_constraint(o, pltpu.VMEM) for o in out]
        out = pl.pallas_call(
            put,
            out_shape=[jax.ShapeDtypeStruct(o.shape, o.dtype) for o in out],
            in_specs=[vmem] * 9,
            out_specs=[hbm] * 9,
            scratch_shapes=[pltpu.SemaphoreType.DMA((4 * layers * 9,))],
            compiler_params=pltpu.CompilerParams(vmem_limit_bytes=VMEM_LIMIT),
        )(*out)
        new = [from_tiles(o.reshape(layers, group, tiles, 8, 128), group * s[1], s[2]) for o, s in zip(out[:3], shapes, strict=True)]
        moved = [from_tiles(o.reshape(layers, 1, tiles, 8, 128), s[1], s[2]) for o, s in zip(out[3:9], shapes * 2, strict=True)]
        return (*new, *moved)

    all_of, cut = P(None, None, None), P(None, "dp", None)
    return jax.shard_map(
        step,
        mesh=mesh,
        in_specs=(P(("rep", "dp"), None, None, None),) * 3 + (all_of,) * 3 + (cut,) * 6,
        out_specs=(P("rep", None, None),) * 3 + (P("rep", "dp", None),) * 6,
        check_vma=False,
    )
```

```python
import functools
import math

import jax
import jax.numpy as jnp
from jax import lax
from jax.experimental import pallas as pl
from jax.experimental.pallas import tpu as pltpu
from jax.sharding import PartitionSpec as P

F32, BF16 = jnp.float32, jnp.bfloat16
RING = 4
CORES = 2
PER_MATRIX = 2
VMEM_LIMIT = 17050 << 10
EARLY_SLOTS = 2
SLOTS = 3

TURN = {'send_half': (-17.7, 10.6), 'load_half': (-8.4, 10.6), 'load_other': (-8.0, 10.6), 'rs1': (-3.6, 10.6), 'rs1_relay_load': (3.5, 10.6), 'rs1_relay': (5.0, 10.6), 'rs2_load': (12.4, 10.6), 'rs2': (13.3, 10.6), 'rs2_relay': (17.1, 10.6), 'update': (21.6, 10.6), 'ag1_own': (24.0, 12.24), 'ag2_relay': (24.8, 12.24), 'ag1_near': (25.3, 12.24), 'ag1_far': (31.0, 12.24), 'ag1_relay': (44.8, 12.24), 'ag1_relay_far': (48.3, 12.24), 'last': (66.1, 12.24)}


def as_tiles(a, rows):
    *lead, r, c = a.shape
    n = len(lead)
    a = a.reshape(*lead, r // 8, 8, c // 128, 128).transpose(*range(n), n, n + 2, n + 1, n + 3)
    return a.reshape(*lead, r // rows, rows // 8 * (c // 128), 8, 128)


def from_tiles(a, rows, columns):
    lead = a.shape[: a.ndim - 4]
    n = len(lead)
    a = a.reshape(*lead, rows // 8, columns // 128, 8, 128).transpose(*range(n), n, n + 2, n + 1, n + 3)
    return a.reshape(*lead, rows, columns)


def kernel(chunks, *refs):
    g_refs, w_refs, m_refs, v_refs = (refs[i : i + 3] for i in (0, 3, 6, 9))
    out_refs, mo_refs, vo_refs = (refs[i : i + 3] for i in (12, 15, 18))
    half_ref, line_ref = refs[21:23]
    own, early, late, s1, s2, recv, sent, near = refs[23:]

    me = lax.axis_index("dp")
    core, chip = me % CORES, me // CORES
    x, y = chip // RING, chip % RING
    mate = 1 - core

    def place(ra, rb):
        return (x + ra * mate + rb * core) % RING * RING + (y + rb * mate + ra * core) % RING

    chips = [[place(ra, rb) for rb in range(RING)] for ra in range(RING)]
    right, left = chips[1][0] * CORES + core, chips[RING - 1][0] * CORES + core
    up, down = chips[0][1] * CORES + core, chips[0][RING - 1] * CORES + core
    partner = chip * CORES + mate

    barrier = pltpu.get_barrier_semaphore()
    peers = (right, left, up, down, partner)
    for peer in peers:
        pl.semaphore_signal(barrier, inc=1, device_id={"dp": peer}, device_id_type=pl.DeviceIdType.MESH)
    pl.semaphore_wait(barrier, len(peers))

    def copy_to(device, src, dst, send_sem, recv_sem):
        pltpu.make_async_remote_copy(
            src_ref=src, dst_ref=dst, send_sem=send_sem, recv_sem=recv_sem, device_id={"dp": device}, device_id_type=pl.DeviceIdType.MESH
        ).start()

    def wait(ref, sem):
        pltpu.make_async_copy(ref, ref, sem).wait()

    kinds = (
        "half_0", "half_1", "half_2", "half_3", "half_4", "relay_l", "relay_r", "fl_direct", "fl_relay", "fr_direct", "fr_relay", "relay_d",
        "relay_u", "fd_direct", "fd_relay", "fu_direct", "fu_relay", "g2_d", "g2_u", "g2_far_d",
        "g2_far_u", "g1_l0", "g1_l1", "g1_l2", "g1_l3", "g1_r0", "g1_r1", "g1_r2",
        "g1_r3", "far_0", "far_3", "far_1l", "far_1r", "far_2l", "far_2r", "core",
    )

    def rsem(k, kind):
        return recv.at[k, kinds.index(kind)]

    def total(dst, at, sources, tiles, unroll):
        @pl.loop(0, tiles // unroll)
        def _(i):
            parts = [ref[pl.ds(start + i * unroll, unroll)].astype(F32) for ref, start in sources]
            dst[pl.ds(at + i * unroll, unroll)] = functools.reduce(jnp.add, parts).astype(BF16)

    class Chunk:
        pass

    cs = []
    base = 0
    for k, (weight, layer, t0, nt) in enumerate(chunks):
        c = Chunk()
        c.k, c.weight, c.layer, c.t0, c.nt, c.h, c.base = k, weight, layer, t0, nt, nt // 2, base
        c.own, c.s1, c.s2 = own.at[k % SLOTS], s1.at[k % SLOTS], s2.at[k]
        c.early, c.late = early.at[k % EARLY_SLOTS], late.at[k % SLOTS]
        c.half_direct, c.line_direct = k < EARLY_SLOTS, k < SLOTS
        c.landing = c.s1 if c.line_direct else line_ref.at[pl.ds(base // (RING * RING) * 12, 12 * nt)]
        base += RING * RING * nt
        cs.append(c)

    def out_at(c, where, which, t=0, n=None):
        return out_refs[c.weight].at[c.layer, where, which, pl.ds(c.t0 + t, c.nt if n is None else n)]

    def spread(c, where, device, kind, t=0, n=None):
        piece = out_at(c, where, core, t, n)
        copy_to(device, piece, piece, sent.at[c.k, 1], rsem(c.k, kind))

    runs = ((8, 12), (6, 8), (12, 14), (0, 6), (14, 16))

    def other(c, piece):
        if 6 <= piece < 14:
            return c.early, (piece - 6) * c.nt
        return c.late, (piece if piece < 6 else piece - 8) * c.nt

    def half(c, piece):
        return other(c, piece) if c.half_direct else (half_ref, c.base + piece * c.nt)

    def send_half(c):
        for run, (first, end) in enumerate(runs):
            dst, at = half(c, first)

            @pl.loop(first, end)
            def _(i):
                src = g_refs[c.weight].at[c.layer, place(i % RING, i // RING), mate, pl.ds(c.t0, c.nt)]
                copy_to(partner, src, dst.at[pl.ds(at + (i - first) * c.nt, c.nt)], sent.at[c.k, 1], rsem(c.k, f"half_{run}"))

    def load_half(c):
        if c.k >= SLOTS:
            old = cs[c.k - SLOTS]
            n = 14 * old.nt
            wait(half_ref.at[pl.ds(0, n)], sent.at[old.k, 0])

        for run, (first, end) in enumerate(runs):

            @pl.loop(first, end)
            def _(i):
                src = g_refs[c.weight].at[c.layer, place(i // RING, i % RING), core, pl.ds(c.t0, c.nt)]
                pltpu.make_async_copy(src, c.own.at[pl.ds(i * c.nt, c.nt)], near.at[c.k, 9 + run]).start()

    def half_arrived(c, run):
        first, end = runs[run]
        dst, at = half(c, first)
        wait(dst.at[pl.ds(at, (end - first) * c.nt)], rsem(c.k, f"half_{run}"))

    def own_arrived(c, run):
        first, end = runs[run]
        wait(c.own.at[pl.ds(first * c.nt, (end - first) * c.nt)], near.at[c.k, 9 + run])

    def load_other(c):
        nt = c.nt
        if c.half_direct:
            return
        for run in range(len(runs)):
            half_arrived(c, run)
        for i, (dst, to, piece, n) in enumerate(((c.early, 0, 6, 8), (c.late, 0, 0, 6), (c.late, 6, 14, 2))):
            src = half_ref.at[pl.ds(c.base + piece * nt, n * nt)]
            pltpu.make_async_copy(src, dst.at[pl.ds(to * nt, n * nt)], near.at[c.k, (1, 7, 8)[i]]).start()

    def rs1(c):
        nt = c.nt
        if not c.half_direct:
            wait(c.early.at[pl.ds(0, 8 * nt)], near.at[c.k, 1])
        for run, sends in enumerate((((8, right, 0, "relay_l"), (10, left, 2, "relay_r")), ((6, right, 6, "fl_direct"),), ((12, left, 8, "fr_direct"),))):
            own_arrived(c, run)
            if c.half_direct:
                half_arrived(c, run)
            for piece, device, at, kind in sends:
                total(c.own, piece * nt, [(c.own, piece * nt), other(c, piece)], 2 * nt, 13)
                copy_to(device, c.own.at[pl.ds(piece * nt, 2 * nt)], c.landing.at[pl.ds(at * nt, 2 * nt)], sent.at[c.k, 0], rsem(c.k, kind))

    def rs1_relay_load(c):
        n = 4 * c.nt
        if c.line_direct:
            return
        for at, kind in ((0, "relay_l"), (2, "relay_r")):
            wait(c.landing.at[pl.ds(at * c.nt, 2 * c.nt)], rsem(c.k, kind))
        pltpu.make_async_copy(c.landing.at[pl.ds(0, n)], c.s1.at[pl.ds(0, n)], near.at[c.k, 2]).start()

    def rs1_relay(c):
        nt = c.nt
        for run in (3, 4):
            own_arrived(c, run)
            if c.half_direct:
                half_arrived(c, run)
        if not c.half_direct:
            wait(c.late.at[pl.ds(0, 6 * nt)], near.at[c.k, 7])
            wait(c.late.at[pl.ds(6 * nt, 2 * nt)], near.at[c.k, 8])
        if not c.line_direct:
            wait(c.s1.at[pl.ds(0, 4 * nt)], near.at[c.k, 2])
        for piece, device, at, to, kind, kind_to in ((4, right, 0, 4, "relay_l", "fl_relay"), (14, left, 2, 10, "relay_r", "fr_relay")):
            if c.line_direct:
                wait(c.s1.at[pl.ds(at * nt, 2 * nt)], rsem(c.k, kind))
            total(c.s1, at * nt, [(c.own, piece * nt), other(c, piece), (c.s1, at * nt)], 2 * nt, 13)
            copy_to(device, c.s1.at[pl.ds(at * nt, 2 * nt)], c.landing.at[pl.ds(to * nt, 2 * nt)], sent.at[c.k, 0], rsem(c.k, kind_to))

    def line(c, rb, t):
        nt = c.nt
        return [(c.own, rb * nt + t), (c.late, rb * nt + t), (c.s1, (4 + rb) * nt + t), (c.s1, (8 + rb) * nt + t)]

    def line_arrived(c):
        for at, kind in ((4, "fl_relay"), (6, "fl_direct"), (8, "fr_direct"), (10, "fr_relay")):
            wait(c.landing.at[pl.ds(at * c.nt, 2 * c.nt)], rsem(c.k, kind))

    def rs2_load(c):
        nt = c.nt
        if c.line_direct:
            return
        line_arrived(c)
        pltpu.make_async_copy(c.landing.at[pl.ds(4 * nt, 8 * nt)], c.s1.at[pl.ds(4 * nt, 8 * nt)], near.at[c.k, 6]).start()

    def rs2(c):
        nt, h = c.nt, c.h
        if c.line_direct:
            line_arrived(c)
        else:
            wait(c.s1.at[pl.ds(4 * nt, 8 * nt)], near.at[c.k, 6])
        for rb, t, n, device, to, kind in (
            (2, 0, h, up, 0, "relay_d"),
            (2, h, nt - h, down, h, "relay_u"),
            (1, h, nt - h, up, nt + h, "fd_direct"),
            (3, 0, h, down, 2 * nt, "fu_direct"),
        ):
            total(c.own, rb * nt + t, line(c, rb, t), n, 13)
            copy_to(device, c.own.at[pl.ds(rb * nt + t, n)], c.s2.at[pl.ds(to, n)], sent.at[c.k, 0], rsem(c.k, kind))

    def rs2_relay(c):
        nt, h = c.nt, c.h
        for rb, t, n, device, to, kind, kind_to in ((1, 0, h, up, nt, "relay_d", "fd_relay"), (3, h, nt - h, down, 2 * nt + h, "relay_u", "fu_relay")):
            here = c.s2.at[pl.ds(t, n)]
            wait(here, rsem(c.k, kind))
            total(c.s2, t, [*line(c, rb, t), (c.s2, t)], n, 13)
            copy_to(device, here, c.s2.at[pl.ds(to, n)], sent.at[c.k, 1], rsem(c.k, kind_to))

    loaded = set()

    def update(c):
        nt, h = c.nt, c.h
        if c.weight not in loaded:
            loaded.add(c.weight)
            for i, (store, src) in enumerate(state(c.weight)):
                wait(store, near.at[c.weight, 3 + i])
        for at, n, kind in ((nt, h, "fd_relay"), (nt + h, nt - h, "fd_direct"), (2 * nt, h, "fu_direct"), (2 * nt + h, nt - h, "fu_relay")):
            wait(c.s2.at[pl.ds(at, n)], rsem(c.k, kind))
        w_store = out_refs[c.weight].at[c.layer, chip, core]
        m_store, v_store = mo_refs[c.weight].at[c.layer], vo_refs[c.weight].at[c.layer]
        sources = [*line(c, 0, 0), (c.s2, nt), (c.s2, 2 * nt)]
        unroll = 4

        @pl.loop(0, nt // unroll)
        def _(i):
            g = functools.reduce(jnp.add, [ref[pl.ds(start + i * unroll, unroll)].astype(F32) for ref, start in sources])
            g = g.astype(BF16).astype(F32)
            here = pl.ds(c.t0 + i * unroll, unroll)
            w = w_store[here].astype(F32)
            m = 0.9 * m_store[here] + 0.1 * g
            v = 0.95 * v_store[here] + 0.05 * g * g
            step = m * lax.rsqrt(v + 1e-8) + 0.1 * w
            w_store[here] = (w - 0.02 * step).astype(BF16)
            m_store[here] = m
            v_store[here] = v

        spread(c, chip, up, "g2_d")
        spread(c, chip, down, "g2_u")

    def ag1_own(c):
        spread(c, chip, right, "g1_l0")
        spread(c, chip, left, "g1_r0")
        spread(c, chip, partner, "core")

    def arrived(c, where, kind, t=0, n=None):
        wait(out_at(c, where, core, t, n), rsem(c.k, kind))

    def ag2_relay(c):
        arrived(c, chips[0][3], "g2_d")
        spread(c, chips[0][3], up, "g2_far_d", 0, c.h)
        arrived(c, chips[0][1], "g2_u")
        spread(c, chips[0][1], down, "g2_far_u", c.h, c.nt - c.h)

    def ag1_near(c):
        for rb in (3, 1):
            spread(c, chips[0][rb], right, f"g1_l{rb}")
            spread(c, chips[0][rb], left, f"g1_r{rb}")
            spread(c, chips[0][rb], partner, "core")

    def ag1_far(c):
        arrived(c, chips[0][2], "g2_far_d", 0, c.h)
        arrived(c, chips[0][2], "g2_far_u", c.h, c.nt - c.h)
        spread(c, chips[0][2], right, "g1_l2")
        spread(c, chips[0][2], left, "g1_r2")
        spread(c, chips[0][2], partner, "core")

    def relay(c, rb):
        for ra, kind in ((3, f"g1_l{rb}"), (1, f"g1_r{rb}")):
            arrived(c, chips[ra][rb], kind)
        if rb == 0:
            spread(c, chips[3][0], right, "far_0")
        elif rb == 3:
            spread(c, chips[1][3], left, "far_3")
        else:
            spread(c, chips[3][rb], right, f"far_{rb}l", 0, c.h)
            spread(c, chips[1][rb], left, f"far_{rb}r", c.h, c.nt - c.h)
        for ra in (3, 1):
            spread(c, chips[ra][rb], partner, "core")

    def ag1_relay(c):
        for rb in (0, 3, 1):
            relay(c, rb)

    def ag1_relay_far(c):
        relay(c, 2)

    def last(c):
        arrived(c, chips[2][0], "far_0")
        arrived(c, chips[2][3], "far_3")
        for rb in (1, 2):
            arrived(c, chips[2][rb], f"far_{rb}l", 0, c.h)
            arrived(c, chips[2][rb], f"far_{rb}r", c.h, c.nt - c.h)
        for rb in range(RING):
            spread(c, chips[2][rb], partner, "core")

    def state(weight):
        mine = w_refs[weight].at[:, chip, core]
        return ((out_refs[weight].at[:, chip, core], mine), (mo_refs[weight], m_refs[weight]), (vo_refs[weight], v_refs[weight]))

    tasks = dict(
        send_half=send_half, load_half=load_half, load_other=load_other, rs1=rs1,
        rs1_relay_load=rs1_relay_load, rs1_relay=rs1_relay, rs2_load=rs2_load, rs2=rs2, rs2_relay=rs2_relay,
        update=update, ag1_own=ag1_own, ag2_relay=ag2_relay, ag1_near=ag1_near, ag1_far=ag1_far, ag1_relay=ag1_relay,
        ag1_relay_far=ag1_relay_far, last=last,
    )
    rank = {name: i for i, name in enumerate(tasks)}
    order = sorted(((TURN[name][0] + TURN[name][1] * c.k, rank[name], name, c) for name in tasks for c in cs), key=lambda one: one[:2])
    turn = {(name, c.k): i for i, (_, _, name, c) in enumerate(order)}
    for k in range(len(cs)):
        assert turn["load_half", k] < turn["load_other", k]
        assert k < SLOTS or turn["update", k - SLOTS] < turn["load_half", k]
        assert k < EARLY_SLOTS or turn["rs1", k - EARLY_SLOTS] < turn["load_other", k]
    for _, _, name, c in order:
        tasks[name](c)
        if name == "rs1" and c.k == 0:
            for weight in range(3):
                for j, (store, src) in enumerate(state(weight)):
                    pltpu.make_async_copy(src, store, near.at[weight, 3 + j]).start()

    for c in cs:
        here = pl.ds(c.t0, c.nt)
        wait(out_refs[c.weight].at[c.layer, :, mate, here], rsem(c.k, "core"))
        wait(half_ref.at[pl.ds(0, 48 * c.nt)], sent.at[c.k, 1])
        if c.k >= len(cs) - SLOTS:
            wait(half_ref.at[pl.ds(0, 14 * c.nt)], sent.at[c.k, 0])


def put(*refs):
    n = len(refs) // 2
    srcs, dsts, sem = refs[:n], refs[n : 2 * n], refs[2 * n]
    copies = []
    for src, dst in zip(srcs, dsts, strict=True):
        for layer in range(src.shape[0]):
            step = src.shape[1] // 4
            for part in range(4):
                here = pl.ds(part * step, step)
                copies.append(pltpu.make_async_copy(src.at[layer, here], dst.at[layer, here], sem.at[len(copies)]))
    for copy in copies:
        copy.start()
    for copy in copies:
        copy.wait()


def solution(mesh):
    group = mesh.shape["dp"]
    assert group == CORES * RING * RING and math.isqrt(group // CORES) == RING

    def step(*arrays):
        terms, weights, m, v = (arrays[i : i + 3] for i in (0, 3, 6, 9))
        layers = m[0].shape[0]
        shapes = [one.shape for one in m]
        blocks = [as_tiles(t[0], s[1]) for t, s in zip(terms, shapes, strict=True)]
        blocks += [as_tiles(w, s[1]) for w, s in zip(weights, shapes, strict=True)]
        tiles = blocks[0].shape[2]
        blocks = [b.reshape(layers, RING * RING, CORES, tiles, 8, 128) for b in blocks]
        moments = [as_tiles(one, one.shape[1]).reshape(layers, tiles, 8, 128) for one in (*m, *v)]
        nt = tiles // PER_MATRIX
        chunks = [(weight, layer, part * nt, nt) for weight in range(3) for layer in range(layers) for part in range(PER_MATRIX)]
        count = len(chunks)
        whole = pltpu.VMEM(blocks[0].shape, BF16)
        moment = pltpu.VMEM(moments[0].shape, F32)
        hbm, vmem = pl.BlockSpec(memory_space=pltpu.HBM), pl.BlockSpec(memory_space=pltpu.VMEM)
        pieces = RING * RING
        out = pl.pallas_call(
            functools.partial(kernel, chunks),
            out_shape=[whole] * 3
            + [moment] * 6
            + [jax.ShapeDtypeStruct((count * pieces * nt, 8, 128), BF16), jax.ShapeDtypeStruct((count * 12 * nt, 8, 128), BF16)],
            in_specs=[hbm] * 12,
            out_specs=[vmem] * 9 + [hbm] * 2,
            scratch_shapes=[
                pltpu.VMEM((SLOTS, pieces * nt, 8, 128), BF16),
                pltpu.VMEM((EARLY_SLOTS, 8 * nt, 8, 128), BF16),
                pltpu.VMEM((SLOTS, 8 * nt, 8, 128), BF16),
                pltpu.VMEM((SLOTS, 12 * nt, 8, 128), BF16),
                pltpu.VMEM((count, 3 * nt, 8, 128), BF16),
                pltpu.SemaphoreType.DMA((count, 36)),
                pltpu.SemaphoreType.DMA((count, 2)),
                pltpu.SemaphoreType.DMA((count, 14)),
            ],
            compiler_params=pltpu.CompilerParams(collective_id=0, has_side_effects=True, vmem_limit_bytes=VMEM_LIMIT),
        )(*blocks, *moments)[:9]
        out = [pltpu.with_memory_space_constraint(o, pltpu.VMEM) for o in out]
        out = pl.pallas_call(
            put,
            out_shape=[jax.ShapeDtypeStruct(o.shape, o.dtype) for o in out],
            in_specs=[vmem] * 9,
            out_specs=[hbm] * 9,
            scratch_shapes=[pltpu.SemaphoreType.DMA((4 * layers * 9,))],
            compiler_params=pltpu.CompilerParams(vmem_limit_bytes=VMEM_LIMIT),
        )(*out)
        new = [from_tiles(o.reshape(layers, group, tiles, 8, 128), group * s[1], s[2]) for o, s in zip(out[:3], shapes, strict=True)]
        moved = [from_tiles(o.reshape(layers, 1, tiles, 8, 128), s[1], s[2]) for o, s in zip(out[3:9], shapes * 2, strict=True)]
        return (*new, *moved)

    all_of, cut = P(None, None, None), P(None, "dp", None)
    return jax.shard_map(
        step,
        mesh=mesh,
        in_specs=(P(("rep", "dp"), None, None, None),) * 3 + (all_of,) * 3 + (cut,) * 6,
        out_specs=(P("rep", None, None),) * 3 + (P("rep", "dp", None),) * 6,
        check_vma=False,
    )
```

```python
import functools
import math

import jax
import jax.numpy as jnp
from jax import lax
from jax.experimental import pallas as pl
from jax.experimental.pallas import tpu as pltpu
from jax.sharding import PartitionSpec as P

F32, BF16 = jnp.float32, jnp.bfloat16
RING = 4
CORES = 2
PER_MATRIX = 2
VMEM_LIMIT = 17050 << 10
EARLY_SLOTS = 2
SLOTS = 3

TURN = {'send_half': (-12.6, 9.9), 'load_half': (-7.3, 9.9), 'load_other': (-7.1, 9.9), 'rs1': (-3.4, 9.9), 'rs1_relay_load': (4.3, 9.9), 'rs1_relay': (4.9, 9.9), 'rs2_load': (10.7, 9.9), 'rs2': (11.8, 9.9), 'rs2_relay': (18.6, 9.9), 'update': (21.8, 9.9), 'ag1_own': (24.9, 11.13), 'ag2_relay': (26.6, 11.13), 'ag1_near': (27.4, 11.13), 'ag1_far': (34.6, 11.13), 'ag1_relay': (49.9, 11.13), 'ag1_relay_far': (55.7, 11.13), 'last': (74.6, 11.13)}


def as_tiles(a, rows):
    *lead, r, c = a.shape
    n = len(lead)
    a = a.reshape(*lead, r // 8, 8, c // 128, 128).transpose(*range(n), n, n + 2, n + 1, n + 3)
    return a.reshape(*lead, r // rows, rows // 8 * (c // 128), 8, 128)


def from_tiles(a, rows, columns):
    lead = a.shape[: a.ndim - 4]
    n = len(lead)
    a = a.reshape(*lead, rows // 8, columns // 128, 8, 128).transpose(*range(n), n, n + 2, n + 1, n + 3)
    return a.reshape(*lead, rows, columns)


def kernel(chunks, *refs):
    g_refs, w_refs, m_refs, v_refs = (refs[i : i + 3] for i in (0, 3, 6, 9))
    out_refs, mo_refs, vo_refs = (refs[i : i + 3] for i in (12, 15, 18))
    half_ref, line_ref = refs[21:23]
    own, early, late, s1, s2, recv, sent, near = refs[23:]

    me = lax.axis_index("dp")
    core, chip = me % CORES, me // CORES
    x, y = chip // RING, chip % RING
    mate = 1 - core

    def place(ra, rb):
        return (x + ra * mate + rb * core) % RING * RING + (y + rb * mate + ra * core) % RING

    chips = [[place(ra, rb) for rb in range(RING)] for ra in range(RING)]
    right, left = chips[1][0] * CORES + core, chips[RING - 1][0] * CORES + core
    up, down = chips[0][1] * CORES + core, chips[0][RING - 1] * CORES + core
    partner = chip * CORES + mate

    barrier = pltpu.get_barrier_semaphore()
    right_mate, left_mate = chips[1][0] * CORES + mate, chips[RING - 1][0] * CORES + mate
    peers = (right, left, up, down, partner, right_mate, left_mate)
    for peer in peers:
        pl.semaphore_signal(barrier, inc=1, device_id={"dp": peer}, device_id_type=pl.DeviceIdType.MESH)
    pl.semaphore_wait(barrier, len(peers))

    def copy_to(device, src, dst, send_sem, recv_sem):
        pltpu.make_async_remote_copy(
            src_ref=src, dst_ref=dst, send_sem=send_sem, recv_sem=recv_sem, device_id={"dp": device}, device_id_type=pl.DeviceIdType.MESH
        ).start()

    def wait(ref, sem):
        pltpu.make_async_copy(ref, ref, sem).wait()

    kinds = (
        "half_0", "half_1", "half_2", "half_3", "half_4", "half_5", "relay_l", "relay_r", "fl_direct", "fl_relay", "fr_direct", "fr_relay", "relay_d",
        "relay_u", "fd_direct", "fd_relay", "fu_direct", "fu_relay", "g2_d", "g2_u", "g2_far_d",
        "g2_far_u", "g1_l0", "g1_l1", "g1_l2", "g1_l3", "g1_r0", "g1_r1", "g1_r2",
        "g1_r3", "far_0", "far_3", "far_1l", "far_1r", "far_2l", "far_2r", "core",
    )

    def rsem(k, kind):
        return recv.at[k, kinds.index(kind)]

    def total(dst, at, sources, tiles, unroll):
        @pl.loop(0, tiles // unroll)
        def _(i):
            parts = [ref[pl.ds(start + i * unroll, unroll)].astype(F32) for ref, start in sources]
            dst[pl.ds(at + i * unroll, unroll)] = functools.reduce(jnp.add, parts).astype(BF16)

    class Chunk:
        pass

    cs = []
    base = 0
    for k, (weight, layer, t0, nt) in enumerate(chunks):
        c = Chunk()
        c.k, c.weight, c.layer, c.t0, c.nt, c.h, c.base = k, weight, layer, t0, nt, nt // 2, base
        c.own, c.s1, c.s2 = own.at[k % SLOTS], s1.at[k % SLOTS], s2.at[k]
        c.early, c.late = early.at[k % EARLY_SLOTS], late.at[k % SLOTS]
        c.half_direct, c.line_direct = k < EARLY_SLOTS, k < SLOTS
        c.landing = c.s1 if c.line_direct else line_ref.at[pl.ds(base // (RING * RING) * 12, 12 * nt)]
        base += RING * RING * nt
        cs.append(c)

    def out_at(c, where, which, t=0, n=None):
        return out_refs[c.weight].at[c.layer, where, which, pl.ds(c.t0 + t, c.nt if n is None else n)]

    def spread(c, where, device, kind, t=0, n=None):
        piece = out_at(c, where, core, t, n)
        copy_to(device, piece, piece, sent.at[c.k, 1], rsem(c.k, kind))

    runs = ((8, 10), (10, 12), (6, 8), (12, 14), (0, 6), (14, 16))

    def other(c, piece):
        if 6 <= piece < 14:
            return c.early, (piece - 6) * c.nt
        return c.late, (piece if piece < 6 else piece - 8) * c.nt

    def half(c, piece):
        return other(c, piece) if c.half_direct else (half_ref, c.base + piece * c.nt)

    def send_half(c):
        for run, (first, end) in enumerate(runs):
            dst, at = half(c, first)

            @pl.loop(first, end)
            def _(i):
                src = g_refs[c.weight].at[c.layer, place(i % RING, i // RING), mate, pl.ds(c.t0, c.nt)]
                copy_to(partner, src, dst.at[pl.ds(at + (i - first) * c.nt, c.nt)], sent.at[c.k, 1], rsem(c.k, f"half_{run}"))

    def load_half(c):
        if c.k >= SLOTS:
            old = cs[c.k - SLOTS]
            n = 14 * old.nt
            wait(half_ref.at[pl.ds(0, n)], sent.at[old.k, 0])

        for run, (first, end) in enumerate(runs):

            @pl.loop(first, end)
            def _(i):
                src = g_refs[c.weight].at[c.layer, place(i // RING, i % RING), core, pl.ds(c.t0, c.nt)]
                pltpu.make_async_copy(src, c.own.at[pl.ds(i * c.nt, c.nt)], near.at[c.k, 9 + run]).start()

    def half_arrived(c, run):
        first, end = runs[run]
        dst, at = half(c, first)
        wait(dst.at[pl.ds(at, (end - first) * c.nt)], rsem(c.k, f"half_{run}"))

    def own_arrived(c, run):
        first, end = runs[run]
        wait(c.own.at[pl.ds(first * c.nt, (end - first) * c.nt)], near.at[c.k, 9 + run])

    def load_other(c):
        nt = c.nt
        if c.half_direct:
            return
        for run in range(len(runs)):
            half_arrived(c, run)
        for i, (dst, to, piece, n) in enumerate(((c.early, 0, 6, 8), (c.late, 0, 0, 6), (c.late, 6, 14, 2))):
            src = half_ref.at[pl.ds(c.base + piece * nt, n * nt)]
            pltpu.make_async_copy(src, dst.at[pl.ds(to * nt, n * nt)], near.at[c.k, (1, 7, 8)[i]]).start()

    def rs1(c):
        nt = c.nt
        if not c.half_direct:
            wait(c.early.at[pl.ds(0, 8 * nt)], near.at[c.k, 1])
        sends = ((8, right, 0, "relay_l"), (10, left, 2, "relay_r"), (6, right, 6, "fl_direct"), (12, left, 8, "fr_direct"))
        for run, (piece, device, at, kind) in enumerate(sends):
            own_arrived(c, run)
            if c.half_direct:
                half_arrived(c, run)
            total(c.own, piece * nt, [(c.own, piece * nt), other(c, piece)], 2 * nt, 13)
            copy_to(device, c.own.at[pl.ds(piece * nt, 2 * nt)], c.landing.at[pl.ds(at * nt, 2 * nt)], sent.at[c.k, 0], rsem(c.k, kind))

    def rs1_relay_load(c):
        n = 4 * c.nt
        if c.line_direct:
            return
        for at, kind in ((0, "relay_l"), (2, "relay_r")):
            wait(c.landing.at[pl.ds(at * c.nt, 2 * c.nt)], rsem(c.k, kind))
        pltpu.make_async_copy(c.landing.at[pl.ds(0, n)], c.s1.at[pl.ds(0, n)], near.at[c.k, 2]).start()

    def rs1_relay(c):
        nt = c.nt
        for run in (4, 5):
            own_arrived(c, run)
            if c.half_direct:
                half_arrived(c, run)
        if not c.half_direct:
            wait(c.late.at[pl.ds(0, 6 * nt)], near.at[c.k, 7])
            wait(c.late.at[pl.ds(6 * nt, 2 * nt)], near.at[c.k, 8])
        if not c.line_direct:
            wait(c.s1.at[pl.ds(0, 4 * nt)], near.at[c.k, 2])
        for piece, device, at, to, kind, kind_to in ((4, right, 0, 4, "relay_l", "fl_relay"), (14, left, 2, 10, "relay_r", "fr_relay")):
            if c.line_direct:
                wait(c.s1.at[pl.ds(at * nt, 2 * nt)], rsem(c.k, kind))
            total(c.s1, at * nt, [(c.own, piece * nt), other(c, piece), (c.s1, at * nt)], 2 * nt, 13)
            copy_to(device, c.s1.at[pl.ds(at * nt, 2 * nt)], c.landing.at[pl.ds(to * nt, 2 * nt)], sent.at[c.k, 0], rsem(c.k, kind_to))

    def line(c, rb, t):
        nt = c.nt
        return [(c.own, rb * nt + t), (c.late, rb * nt + t), (c.s1, (4 + rb) * nt + t), (c.s1, (8 + rb) * nt + t)]

    def line_arrived(c):
        for at, kind in ((4, "fl_relay"), (6, "fl_direct"), (8, "fr_direct"), (10, "fr_relay")):
            wait(c.landing.at[pl.ds(at * c.nt, 2 * c.nt)], rsem(c.k, kind))

    def rs2_load(c):
        nt = c.nt
        if c.line_direct:
            return
        line_arrived(c)
        pltpu.make_async_copy(c.landing.at[pl.ds(4 * nt, 8 * nt)], c.s1.at[pl.ds(4 * nt, 8 * nt)], near.at[c.k, 6]).start()

    def rs2(c):
        nt, h = c.nt, c.h
        if c.line_direct:
            line_arrived(c)
        else:
            wait(c.s1.at[pl.ds(4 * nt, 8 * nt)], near.at[c.k, 6])
        for rb, t, n, device, to, kind in (
            (2, 0, h, up, 0, "relay_d"),
            (2, h, nt - h, down, h, "relay_u"),
            (1, h, nt - h, up, nt + h, "fd_direct"),
            (3, 0, h, down, 2 * nt, "fu_direct"),
        ):
            total(c.own, rb * nt + t, line(c, rb, t), n, 13)
            copy_to(device, c.own.at[pl.ds(rb * nt + t, n)], c.s2.at[pl.ds(to, n)], sent.at[c.k, 0], rsem(c.k, kind))

    def rs2_relay(c):
        nt, h = c.nt, c.h
        for rb, t, n, device, to, kind, kind_to in ((1, 0, h, up, nt, "relay_d", "fd_relay"), (3, h, nt - h, down, 2 * nt + h, "relay_u", "fu_relay")):
            here = c.s2.at[pl.ds(t, n)]
            wait(here, rsem(c.k, kind))
            total(c.s2, t, [*line(c, rb, t), (c.s2, t)], n, 13)
            copy_to(device, here, c.s2.at[pl.ds(to, n)], sent.at[c.k, 1], rsem(c.k, kind_to))

    loaded = set()

    def update(c):
        nt, h = c.nt, c.h
        if c.weight not in loaded:
            loaded.add(c.weight)
            for i, (store, src) in enumerate(state(c.weight)):
                wait(store, near.at[c.weight, 3 + i])
        for at, n, kind in ((nt, h, "fd_relay"), (nt + h, nt - h, "fd_direct"), (2 * nt, h, "fu_direct"), (2 * nt + h, nt - h, "fu_relay")):
            wait(c.s2.at[pl.ds(at, n)], rsem(c.k, kind))
        w_store = out_refs[c.weight].at[c.layer, chip, core]
        m_store, v_store = mo_refs[c.weight].at[c.layer], vo_refs[c.weight].at[c.layer]
        sources = [*line(c, 0, 0), (c.s2, nt), (c.s2, 2 * nt)]
        unroll = 4

        @pl.loop(0, nt // unroll)
        def _(i):
            g = functools.reduce(jnp.add, [ref[pl.ds(start + i * unroll, unroll)].astype(F32) for ref, start in sources])
            g = g.astype(BF16).astype(F32)
            here = pl.ds(c.t0 + i * unroll, unroll)
            w = w_store[here].astype(F32)
            m = 0.9 * m_store[here] + 0.1 * g
            v = 0.95 * v_store[here] + 0.05 * g * g
            step = m * lax.rsqrt(v + 1e-8) + 0.1 * w
            w_store[here] = (w - 0.02 * step).astype(BF16)
            m_store[here] = m
            v_store[here] = v

        spread(c, chip, up, "g2_d")
        spread(c, chip, down, "g2_u")

    def ag1_own(c):
        spread(c, chip, right, "g1_l0")
        spread(c, chip, left, "g1_r0")
        spread(c, chip, partner, "core")

    def arrived(c, where, kind, t=0, n=None):
        wait(out_at(c, where, core, t, n), rsem(c.k, kind))

    def ag2_relay(c):
        arrived(c, chips[0][3], "g2_d")
        spread(c, chips[0][3], up, "g2_far_d", 0, c.h)
        arrived(c, chips[0][1], "g2_u")
        spread(c, chips[0][1], down, "g2_far_u", c.h, c.nt - c.h)

    def ag1_near(c):
        for rb in (3, 1):
            spread(c, chips[0][rb], right, f"g1_l{rb}")
            spread(c, chips[0][rb], left, f"g1_r{rb}")
            spread(c, chips[0][rb], partner, "core")

    def ag1_far(c):
        arrived(c, chips[0][2], "g2_far_d", 0, c.h)
        arrived(c, chips[0][2], "g2_far_u", c.h, c.nt - c.h)
        spread(c, chips[0][2], right, "g1_l2")
        spread(c, chips[0][2], left, "g1_r2")
        spread(c, chips[0][2], partner, "core")

    def straight(c, rb):
        return rb == 2 and c is cs[-1]

    def relay(c, rb):
        for ra, kind in ((3, f"g1_l{rb}"), (1, f"g1_r{rb}")):
            arrived(c, chips[ra][rb], kind)
        if rb == 0:
            spread(c, chips[3][0], right, "far_0")
        elif rb == 3:
            spread(c, chips[1][3], left, "far_3")
        else:
            spread(c, chips[3][rb], right, f"far_{rb}l", 0, c.h)
            spread(c, chips[1][rb], left, f"far_{rb}r", c.h, c.nt - c.h)
            if straight(c, rb):
                spread(c, chips[3][rb], right_mate, "core", 0, c.h)
                spread(c, chips[1][rb], left_mate, "core", c.h, c.nt - c.h)
        for ra in (3, 1):
            spread(c, chips[ra][rb], partner, "core")

    def ag1_relay(c):
        for rb in (0, 3, 1):
            relay(c, rb)

    def ag1_relay_far(c):
        relay(c, 2)

    def last(c):
        for rb in (0, 3, 1, 2):
            if rb in (0, 3):
                arrived(c, chips[2][rb], f"far_{rb}")
            else:
                arrived(c, chips[2][rb], f"far_{rb}l", 0, c.h)
                arrived(c, chips[2][rb], f"far_{rb}r", c.h, c.nt - c.h)
            if not straight(c, rb):
                spread(c, chips[2][rb], partner, "core")

    def state(weight):
        mine = w_refs[weight].at[:, chip, core]
        return ((out_refs[weight].at[:, chip, core], mine), (mo_refs[weight], m_refs[weight]), (vo_refs[weight], v_refs[weight]))

    tasks = dict(
        send_half=send_half, load_half=load_half, load_other=load_other, rs1=rs1,
        rs1_relay_load=rs1_relay_load, rs1_relay=rs1_relay, rs2_load=rs2_load, rs2=rs2, rs2_relay=rs2_relay,
        update=update, ag1_own=ag1_own, ag2_relay=ag2_relay, ag1_near=ag1_near, ag1_far=ag1_far, ag1_relay=ag1_relay,
        ag1_relay_far=ag1_relay_far, last=last,
    )
    rank = {name: i for i, name in enumerate(tasks)}
    order = sorted(((TURN[name][0] + TURN[name][1] * c.k, rank[name], name, c) for name in tasks for c in cs), key=lambda one: one[:2])
    turn = {(name, c.k): i for i, (_, _, name, c) in enumerate(order)}
    for k in range(len(cs)):
        assert turn["load_half", k] < turn["load_other", k]
        assert k < SLOTS or turn["update", k - SLOTS] < turn["load_half", k]
        assert k < EARLY_SLOTS or turn["rs1", k - EARLY_SLOTS] < turn["load_other", k]
    for _, _, name, c in order:
        tasks[name](c)
        if name == "rs1" and c.k == 0:
            for weight in range(3):
                for j, (store, src) in enumerate(state(weight)):
                    pltpu.make_async_copy(src, store, near.at[weight, 3 + j]).start()

    for c in cs:
        here = pl.ds(c.t0, c.nt)
        wait(out_refs[c.weight].at[c.layer, :, mate, here], rsem(c.k, "core"))
        wait(half_ref.at[pl.ds(0, 48 * c.nt)], sent.at[c.k, 1])
        if c.k >= len(cs) - SLOTS:
            wait(half_ref.at[pl.ds(0, 14 * c.nt)], sent.at[c.k, 0])


def put(*refs):
    n = len(refs) // 2
    srcs, dsts, sem = refs[:n], refs[n : 2 * n], refs[2 * n]
    copies = []
    for src, dst in zip(srcs, dsts, strict=True):
        for layer in range(src.shape[0]):
            step = src.shape[1] // 4
            for part in range(4):
                here = pl.ds(part * step, step)
                copies.append(pltpu.make_async_copy(src.at[layer, here], dst.at[layer, here], sem.at[len(copies)]))
    for copy in copies:
        copy.start()
    for copy in copies:
        copy.wait()


def solution(mesh):
    group = mesh.shape["dp"]
    assert group == CORES * RING * RING and math.isqrt(group // CORES) == RING

    def step(*arrays):
        terms, weights, m, v = (arrays[i : i + 3] for i in (0, 3, 6, 9))
        layers = m[0].shape[0]
        shapes = [one.shape for one in m]
        blocks = [as_tiles(t[0], s[1]) for t, s in zip(terms, shapes, strict=True)]
        blocks += [as_tiles(w, s[1]) for w, s in zip(weights, shapes, strict=True)]
        tiles = blocks[0].shape[2]
        blocks = [b.reshape(layers, RING * RING, CORES, tiles, 8, 128) for b in blocks]
        moments = [as_tiles(one, one.shape[1]).reshape(layers, tiles, 8, 128) for one in (*m, *v)]
        nt = tiles // PER_MATRIX
        chunks = [(weight, layer, part * nt, nt) for weight in range(3) for layer in range(layers) for part in range(PER_MATRIX)]
        count = len(chunks)
        whole = pltpu.VMEM(blocks[0].shape, BF16)
        moment = pltpu.VMEM(moments[0].shape, F32)
        hbm, vmem = pl.BlockSpec(memory_space=pltpu.HBM), pl.BlockSpec(memory_space=pltpu.VMEM)
        pieces = RING * RING
        out = pl.pallas_call(
            functools.partial(kernel, chunks),
            out_shape=[whole] * 3
            + [moment] * 6
            + [jax.ShapeDtypeStruct((count * pieces * nt, 8, 128), BF16), jax.ShapeDtypeStruct((count * 12 * nt, 8, 128), BF16)],
            in_specs=[hbm] * 12,
            out_specs=[vmem] * 9 + [hbm] * 2,
            scratch_shapes=[
                pltpu.VMEM((SLOTS, pieces * nt, 8, 128), BF16),
                pltpu.VMEM((EARLY_SLOTS, 8 * nt, 8, 128), BF16),
                pltpu.VMEM((SLOTS, 8 * nt, 8, 128), BF16),
                pltpu.VMEM((SLOTS, 12 * nt, 8, 128), BF16),
                pltpu.VMEM((count, 3 * nt, 8, 128), BF16),
                pltpu.SemaphoreType.DMA((count, 37)),
                pltpu.SemaphoreType.DMA((count, 2)),
                pltpu.SemaphoreType.DMA((count, 15)),
            ],
            compiler_params=pltpu.CompilerParams(collective_id=0, has_side_effects=True, vmem_limit_bytes=VMEM_LIMIT),
        )(*blocks, *moments)[:9]
        out = [pltpu.with_memory_space_constraint(o, pltpu.VMEM) for o in out]
        out = pl.pallas_call(
            put,
            out_shape=[jax.ShapeDtypeStruct(o.shape, o.dtype) for o in out],
            in_specs=[vmem] * 9,
            out_specs=[hbm] * 9,
            scratch_shapes=[pltpu.SemaphoreType.DMA((4 * layers * 9,))],
            compiler_params=pltpu.CompilerParams(vmem_limit_bytes=VMEM_LIMIT),
        )(*out)
        new = [from_tiles(o.reshape(layers, group, tiles, 8, 128), group * s[1], s[2]) for o, s in zip(out[:3], shapes, strict=True)]
        moved = [from_tiles(o.reshape(layers, 1, tiles, 8, 128), s[1], s[2]) for o, s in zip(out[3:9], shapes * 2, strict=True)]
        return (*new, *moved)

    all_of, cut = P(None, None, None), P(None, "dp", None)
    return jax.shard_map(
        step,
        mesh=mesh,
        in_specs=(P(("rep", "dp"), None, None, None),) * 3 + (all_of,) * 3 + (cut,) * 6,
        out_specs=(P("rep", None, None),) * 3 + (P("rep", "dp", None),) * 6,
        check_vma=False,
    )
```

```python
import functools
import math

import jax
import jax.numpy as jnp
from jax import lax
from jax.experimental import pallas as pl
from jax.experimental.pallas import tpu as pltpu
from jax.sharding import PartitionSpec as P

F32, BF16 = jnp.float32, jnp.bfloat16
RING = 4
CORES = 2
PER_MATRIX = 2
VMEM_LIMIT = 17050 << 10
EARLY_SLOTS = 2
AHEAD = 2
SLOTS = 3

TURN = {'send_half': (-12.6, 9.9), 'load_half': (-7.3, 9.9), 'load_other': (-7.1, 9.9), 'rs1': (-3.4, 9.9), 'rs1_relay_load': (4.3, 9.9), 'rs1_relay': (4.9, 9.9), 'rs2_load': (10.7, 9.9), 'rs2': (11.8, 9.9), 'rs2_relay': (18.6, 9.9), 'update': (21.8, 9.9), 'ag1_own': (24.9, 11.13), 'ag2_relay': (26.6, 11.13), 'ag1_near': (27.4, 11.13), 'ag1_far': (34.6, 11.13), 'ag1_relay': (49.9, 11.13), 'ag1_relay_far': (55.7, 11.13), 'last': (74.6, 11.13)}


def as_tiles(a, rows):
    *lead, r, c = a.shape
    n = len(lead)
    a = a.reshape(*lead, r // 8, 8, c // 128, 128).transpose(*range(n), n, n + 2, n + 1, n + 3)
    return a.reshape(*lead, r // rows, rows // 8 * (c // 128), 8, 128)


def from_tiles(a, rows, columns):
    lead = a.shape[: a.ndim - 4]
    n = len(lead)
    a = a.reshape(*lead, rows // 8, columns // 128, 8, 128).transpose(*range(n), n, n + 2, n + 1, n + 3)
    return a.reshape(*lead, rows, columns)


def kernel(chunks, *refs):
    g_refs, w_refs, m_refs, v_refs = (refs[i : i + 3] for i in (0, 3, 6, 9))
    out_refs, mo_refs, vo_refs = (refs[i : i + 3] for i in (12, 15, 18))
    half_ref, line_ref = refs[21:23]
    own, early, late, s1, s2, recv, sent, near = refs[23:]

    me = lax.axis_index("dp")
    core, chip = me % CORES, me // CORES
    x, y = chip // RING, chip % RING
    mate = 1 - core

    def place(ra, rb):
        return (x + ra * mate + rb * core) % RING * RING + (y + rb * mate + ra * core) % RING

    chips = [[place(ra, rb) for rb in range(RING)] for ra in range(RING)]
    right, left = chips[1][0] * CORES + core, chips[RING - 1][0] * CORES + core
    up, down = chips[0][1] * CORES + core, chips[0][RING - 1] * CORES + core
    partner = chip * CORES + mate

    barrier = pltpu.get_barrier_semaphore()
    right_mate, left_mate = chips[1][0] * CORES + mate, chips[RING - 1][0] * CORES + mate
    peers = (right, left, up, down, partner, right_mate, left_mate)
    for peer in peers:
        pl.semaphore_signal(barrier, inc=1, device_id={"dp": peer}, device_id_type=pl.DeviceIdType.MESH)

    def copy_to(device, src, dst, send_sem, recv_sem):
        pltpu.make_async_remote_copy(
            src_ref=src, dst_ref=dst, send_sem=send_sem, recv_sem=recv_sem, device_id={"dp": device}, device_id_type=pl.DeviceIdType.MESH
        ).start()

    def wait(ref, sem):
        pltpu.make_async_copy(ref, ref, sem).wait()

    kinds = (
        "half_0", "half_1", "half_2", "half_3", "half_4", "half_5", "relay_l", "relay_r", "fl_direct", "fl_relay", "fr_direct", "fr_relay", "relay_d",
        "relay_u", "fd_direct", "fd_relay", "fu_direct", "fu_relay", "g2_d", "g2_u", "g2_far_d",
        "g2_far_u", "g1_l0", "g1_l1", "g1_l2", "g1_l3", "g1_r0", "g1_r1", "g1_r2",
        "g1_r3", "far_0", "far_3", "far_1l", "far_1r", "far_2l", "far_2r", "core",
    )

    def rsem(k, kind):
        return recv.at[k, kinds.index(kind)]

    def total(dst, at, sources, tiles, unroll):
        @pl.loop(0, tiles // unroll)
        def _(i):
            parts = [ref[pl.ds(start + i * unroll, unroll)].astype(F32) for ref, start in sources]
            dst[pl.ds(at + i * unroll, unroll)] = functools.reduce(jnp.add, parts).astype(BF16)

    class Chunk:
        pass

    cs = []
    base = 0
    for k, (weight, layer, t0, nt) in enumerate(chunks):
        c = Chunk()
        c.k, c.weight, c.layer, c.t0, c.nt, c.h, c.base = k, weight, layer, t0, nt, nt // 2, base
        c.own, c.s1, c.s2 = own.at[k % SLOTS], s1.at[k % SLOTS], s2.at[k]
        c.early, c.late = early.at[k % EARLY_SLOTS], late.at[k % SLOTS]
        c.half_direct, c.line_direct = k < EARLY_SLOTS, k < SLOTS
        c.landing = c.s1 if c.line_direct else line_ref.at[pl.ds(base // (RING * RING) * 12, 12 * nt)]
        base += RING * RING * nt
        cs.append(c)

    def out_at(c, where, which, t=0, n=None):
        return out_refs[c.weight].at[c.layer, where, which, pl.ds(c.t0 + t, c.nt if n is None else n)]

    def spread(c, where, device, kind, t=0, n=None):
        piece = out_at(c, where, core, t, n)
        copy_to(device, piece, piece, sent.at[c.k, 1], rsem(c.k, kind))

    runs = ((8, 10), (10, 12), (6, 8), (12, 14), (0, 6), (14, 16))

    def other(c, piece):
        if 6 <= piece < 14:
            return c.early, (piece - 6) * c.nt
        return c.late, (piece if piece < 6 else piece - 8) * c.nt

    def half(c, piece):
        return other(c, piece) if c.half_direct else (half_ref, c.base + piece * c.nt)

    def send_half(c):
        for run, (first, end) in enumerate(runs):
            dst, at = half(c, first)
            if c.k == 0 and run < AHEAD:
                n = (end - first) * c.nt
                wait(ahead(run, n), near.at[0, 15 + run])
                copy_to(partner, ahead(run, n), dst.at[pl.ds(at, n)], sent.at[0, 2], rsem(0, f"half_{run}"))
                continue

            @pl.loop(first, end)
            def _(i):
                src = g_refs[c.weight].at[c.layer, place(i % RING, i // RING), mate, pl.ds(c.t0, c.nt)]
                copy_to(partner, src, dst.at[pl.ds(at + (i - first) * c.nt, c.nt)], sent.at[c.k, 1], rsem(c.k, f"half_{run}"))

    def ahead(run, n):
        return own.at[SLOTS - 1, pl.ds(2 * run * cs[0].nt, n)]

    def load_ahead(c):
        for run, (first, end) in enumerate(runs[:AHEAD]):

            @pl.loop(first, end)
            def _(i):
                src = g_refs[c.weight].at[c.layer, place(i % RING, i // RING), mate, pl.ds(c.t0, c.nt)]
                pltpu.make_async_copy(src, ahead(run, 2 * c.nt).at[pl.ds((i - first) * c.nt, c.nt)], near.at[0, 15 + run]).start()

    def load_half(c):
        if c.k == SLOTS - 1:
            wait(half_ref.at[pl.ds(0, 2 * AHEAD * cs[0].nt)], sent.at[0, 2])
        if c.k >= SLOTS:
            old = cs[c.k - SLOTS]
            n = 14 * old.nt
            wait(half_ref.at[pl.ds(0, n)], sent.at[old.k, 0])

        for run, (first, end) in enumerate(runs):

            @pl.loop(first, end)
            def _(i):
                src = g_refs[c.weight].at[c.layer, place(i // RING, i % RING), core, pl.ds(c.t0, c.nt)]
                pltpu.make_async_copy(src, c.own.at[pl.ds(i * c.nt, c.nt)], near.at[c.k, 9 + run]).start()

    def half_arrived(c, run):
        first, end = runs[run]
        dst, at = half(c, first)
        wait(dst.at[pl.ds(at, (end - first) * c.nt)], rsem(c.k, f"half_{run}"))

    def own_arrived(c, run):
        first, end = runs[run]
        wait(c.own.at[pl.ds(first * c.nt, (end - first) * c.nt)], near.at[c.k, 9 + run])

    def load_other(c):
        nt = c.nt
        if c.half_direct:
            return
        for run in range(len(runs)):
            half_arrived(c, run)
        for i, (dst, to, piece, n) in enumerate(((c.early, 0, 6, 8), (c.late, 0, 0, 6), (c.late, 6, 14, 2))):
            src = half_ref.at[pl.ds(c.base + piece * nt, n * nt)]
            pltpu.make_async_copy(src, dst.at[pl.ds(to * nt, n * nt)], near.at[c.k, (1, 7, 8)[i]]).start()

    def rs1(c):
        nt = c.nt
        if not c.half_direct:
            wait(c.early.at[pl.ds(0, 8 * nt)], near.at[c.k, 1])
        sends = ((8, right, 0, "relay_l"), (10, left, 2, "relay_r"), (6, right, 6, "fl_direct"), (12, left, 8, "fr_direct"))
        for run, (piece, device, at, kind) in enumerate(sends):
            own_arrived(c, run)
            if c.half_direct:
                half_arrived(c, run)
            total(c.own, piece * nt, [(c.own, piece * nt), other(c, piece)], 2 * nt, 13)
            copy_to(device, c.own.at[pl.ds(piece * nt, 2 * nt)], c.landing.at[pl.ds(at * nt, 2 * nt)], sent.at[c.k, 0], rsem(c.k, kind))

    def rs1_relay_load(c):
        n = 4 * c.nt
        if c.line_direct:
            return
        for at, kind in ((0, "relay_l"), (2, "relay_r")):
            wait(c.landing.at[pl.ds(at * c.nt, 2 * c.nt)], rsem(c.k, kind))
        pltpu.make_async_copy(c.landing.at[pl.ds(0, n)], c.s1.at[pl.ds(0, n)], near.at[c.k, 2]).start()

    def rs1_relay(c):
        nt = c.nt
        for run in (4, 5):
            own_arrived(c, run)
            if c.half_direct:
                half_arrived(c, run)
        if not c.half_direct:
            wait(c.late.at[pl.ds(0, 6 * nt)], near.at[c.k, 7])
            wait(c.late.at[pl.ds(6 * nt, 2 * nt)], near.at[c.k, 8])
        if not c.line_direct:
            wait(c.s1.at[pl.ds(0, 4 * nt)], near.at[c.k, 2])
        for piece, device, at, to, kind, kind_to in ((4, right, 0, 4, "relay_l", "fl_relay"), (14, left, 2, 10, "relay_r", "fr_relay")):
            if c.line_direct:
                wait(c.s1.at[pl.ds(at * nt, 2 * nt)], rsem(c.k, kind))
            total(c.s1, at * nt, [(c.own, piece * nt), other(c, piece), (c.s1, at * nt)], 2 * nt, 13)
            copy_to(device, c.s1.at[pl.ds(at * nt, 2 * nt)], c.landing.at[pl.ds(to * nt, 2 * nt)], sent.at[c.k, 0], rsem(c.k, kind_to))

    def line(c, rb, t):
        nt = c.nt
        return [(c.own, rb * nt + t), (c.late, rb * nt + t), (c.s1, (4 + rb) * nt + t), (c.s1, (8 + rb) * nt + t)]

    def line_arrived(c):
        for at, kind in ((4, "fl_relay"), (6, "fl_direct"), (8, "fr_direct"), (10, "fr_relay")):
            wait(c.landing.at[pl.ds(at * c.nt, 2 * c.nt)], rsem(c.k, kind))

    def rs2_load(c):
        nt = c.nt
        if c.line_direct:
            return
        line_arrived(c)
        pltpu.make_async_copy(c.landing.at[pl.ds(4 * nt, 8 * nt)], c.s1.at[pl.ds(4 * nt, 8 * nt)], near.at[c.k, 6]).start()

    def rs2(c):
        nt, h = c.nt, c.h
        if c.line_direct:
            line_arrived(c)
        else:
            wait(c.s1.at[pl.ds(4 * nt, 8 * nt)], near.at[c.k, 6])
        for rb, t, n, device, to, kind in (
            (2, 0, h, up, 0, "relay_d"),
            (2, h, nt - h, down, h, "relay_u"),
            (1, h, nt - h, up, nt + h, "fd_direct"),
            (3, 0, h, down, 2 * nt, "fu_direct"),
        ):
            total(c.own, rb * nt + t, line(c, rb, t), n, 13)
            copy_to(device, c.own.at[pl.ds(rb * nt + t, n)], c.s2.at[pl.ds(to, n)], sent.at[c.k, 0], rsem(c.k, kind))

    def rs2_relay(c):
        nt, h = c.nt, c.h
        for rb, t, n, device, to, kind, kind_to in ((1, 0, h, up, nt, "relay_d", "fd_relay"), (3, h, nt - h, down, 2 * nt + h, "relay_u", "fu_relay")):
            here = c.s2.at[pl.ds(t, n)]
            wait(here, rsem(c.k, kind))
            total(c.s2, t, [*line(c, rb, t), (c.s2, t)], n, 13)
            copy_to(device, here, c.s2.at[pl.ds(to, n)], sent.at[c.k, 1], rsem(c.k, kind_to))

    loaded = set()

    def update(c):
        nt, h = c.nt, c.h
        if c.weight not in loaded:
            loaded.add(c.weight)
            for i, (store, src) in enumerate(state(c.weight)):
                wait(store, near.at[c.weight, 3 + i])
        for at, n, kind in ((nt, h, "fd_relay"), (nt + h, nt - h, "fd_direct"), (2 * nt, h, "fu_direct"), (2 * nt + h, nt - h, "fu_relay")):
            wait(c.s2.at[pl.ds(at, n)], rsem(c.k, kind))
        w_store = out_refs[c.weight].at[c.layer, chip, core]
        m_store, v_store = mo_refs[c.weight].at[c.layer], vo_refs[c.weight].at[c.layer]
        sources = [*line(c, 0, 0), (c.s2, nt), (c.s2, 2 * nt)]
        unroll = 4

        @pl.loop(0, nt // unroll)
        def _(i):
            g = functools.reduce(jnp.add, [ref[pl.ds(start + i * unroll, unroll)].astype(F32) for ref, start in sources])
            g = g.astype(BF16).astype(F32)
            here = pl.ds(c.t0 + i * unroll, unroll)
            w = w_store[here].astype(F32)
            m = 0.9 * m_store[here] + 0.1 * g
            v = 0.95 * v_store[here] + 0.05 * g * g
            step = m * lax.rsqrt(v + 1e-8) + 0.1 * w
            w_store[here] = (w - 0.02 * step).astype(BF16)
            m_store[here] = m
            v_store[here] = v

        spread(c, chip, up, "g2_d")
        spread(c, chip, down, "g2_u")

    def ag1_own(c):
        spread(c, chip, right, "g1_l0")
        spread(c, chip, left, "g1_r0")
        spread(c, chip, partner, "core")

    def arrived(c, where, kind, t=0, n=None):
        wait(out_at(c, where, core, t, n), rsem(c.k, kind))

    def ag2_relay(c):
        arrived(c, chips[0][3], "g2_d")
        spread(c, chips[0][3], up, "g2_far_d", 0, c.h)
        arrived(c, chips[0][1], "g2_u")
        spread(c, chips[0][1], down, "g2_far_u", c.h, c.nt - c.h)

    def ag1_near(c):
        for rb in (3, 1):
            spread(c, chips[0][rb], right, f"g1_l{rb}")
            spread(c, chips[0][rb], left, f"g1_r{rb}")
            spread(c, chips[0][rb], partner, "core")

    def ag1_far(c):
        arrived(c, chips[0][2], "g2_far_d", 0, c.h)
        arrived(c, chips[0][2], "g2_far_u", c.h, c.nt - c.h)
        spread(c, chips[0][2], right, "g1_l2")
        spread(c, chips[0][2], left, "g1_r2")
        spread(c, chips[0][2], partner, "core")

    def straight(c, rb):
        return rb == 2 and c is cs[-1]

    def relay(c, rb):
        for ra, kind in ((3, f"g1_l{rb}"), (1, f"g1_r{rb}")):
            arrived(c, chips[ra][rb], kind)
        if rb == 0:
            spread(c, chips[3][0], right, "far_0")
        elif rb == 3:
            spread(c, chips[1][3], left, "far_3")
        else:
            spread(c, chips[3][rb], right, f"far_{rb}l", 0, c.h)
            spread(c, chips[1][rb], left, f"far_{rb}r", c.h, c.nt - c.h)
            if straight(c, rb):
                spread(c, chips[3][rb], right_mate, "core", 0, c.h)
                spread(c, chips[1][rb], left_mate, "core", c.h, c.nt - c.h)
        for ra in (3, 1):
            spread(c, chips[ra][rb], partner, "core")

    def ag1_relay(c):
        for rb in (0, 3, 1):
            relay(c, rb)

    def ag1_relay_far(c):
        relay(c, 2)

    def last(c):
        for rb in (0, 3, 1, 2):
            if rb in (0, 3):
                arrived(c, chips[2][rb], f"far_{rb}")
            else:
                arrived(c, chips[2][rb], f"far_{rb}l", 0, c.h)
                arrived(c, chips[2][rb], f"far_{rb}r", c.h, c.nt - c.h)
            if not straight(c, rb):
                spread(c, chips[2][rb], partner, "core")

    def state(weight):
        mine = w_refs[weight].at[:, chip, core]
        return ((out_refs[weight].at[:, chip, core], mine), (mo_refs[weight], m_refs[weight]), (vo_refs[weight], v_refs[weight]))

    tasks = dict(
        send_half=send_half, load_half=load_half, load_other=load_other, rs1=rs1,
        rs1_relay_load=rs1_relay_load, rs1_relay=rs1_relay, rs2_load=rs2_load, rs2=rs2, rs2_relay=rs2_relay,
        update=update, ag1_own=ag1_own, ag2_relay=ag2_relay, ag1_near=ag1_near, ag1_far=ag1_far, ag1_relay=ag1_relay,
        ag1_relay_far=ag1_relay_far, last=last,
    )
    rank = {name: i for i, name in enumerate(tasks)}
    order = sorted(((TURN[name][0] + TURN[name][1] * c.k, rank[name], name, c) for name in tasks for c in cs), key=lambda one: one[:2])
    turn = {(name, c.k): i for i, (_, _, name, c) in enumerate(order)}
    for k in range(len(cs)):
        assert turn["load_half", k] < turn["load_other", k]
        assert k < SLOTS or turn["update", k - SLOTS] < turn["load_half", k]
        assert k < EARLY_SLOTS or turn["rs1", k - EARLY_SLOTS] < turn["load_other", k]
    load_ahead(cs[0])
    load_half(cs[0])
    pl.semaphore_wait(barrier, len(peers))
    for _, _, name, c in order:
        if name != "load_half" or c.k > 0:
            tasks[name](c)
        if name == "rs1" and c.k == 0:
            for weight in range(3):
                for j, (store, src) in enumerate(state(weight)):
                    pltpu.make_async_copy(src, store, near.at[weight, 3 + j]).start()

    for c in cs:
        here = pl.ds(c.t0, c.nt)
        wait(out_refs[c.weight].at[c.layer, :, mate, here], rsem(c.k, "core"))
        wait(half_ref.at[pl.ds(0, (48 if c.k else 48 - 2 * AHEAD) * c.nt)], sent.at[c.k, 1])
        if c.k >= len(cs) - SLOTS:
            wait(half_ref.at[pl.ds(0, 14 * c.nt)], sent.at[c.k, 0])


def put(*refs):
    n = len(refs) // 2
    srcs, dsts, sem = refs[:n], refs[n : 2 * n], refs[2 * n]
    copies = []
    for src, dst in zip(srcs, dsts, strict=True):
        for layer in range(src.shape[0]):
            step = src.shape[1] // 4
            for part in range(4):
                here = pl.ds(part * step, step)
                copies.append(pltpu.make_async_copy(src.at[layer, here], dst.at[layer, here], sem.at[len(copies)]))
    for copy in copies:
        copy.start()
    for copy in copies:
        copy.wait()


def solution(mesh):
    group = mesh.shape["dp"]
    assert group == CORES * RING * RING and math.isqrt(group // CORES) == RING

    def step(*arrays):
        terms, weights, m, v = (arrays[i : i + 3] for i in (0, 3, 6, 9))
        layers = m[0].shape[0]
        shapes = [one.shape for one in m]
        blocks = [as_tiles(t[0], s[1]) for t, s in zip(terms, shapes, strict=True)]
        blocks += [as_tiles(w, s[1]) for w, s in zip(weights, shapes, strict=True)]
        tiles = blocks[0].shape[2]
        blocks = [b.reshape(layers, RING * RING, CORES, tiles, 8, 128) for b in blocks]
        moments = [as_tiles(one, one.shape[1]).reshape(layers, tiles, 8, 128) for one in (*m, *v)]
        nt = tiles // PER_MATRIX
        chunks = [(weight, layer, part * nt, nt) for weight in range(3) for layer in range(layers) for part in range(PER_MATRIX)]
        count = len(chunks)
        whole = pltpu.VMEM(blocks[0].shape, BF16)
        moment = pltpu.VMEM(moments[0].shape, F32)
        hbm, vmem = pl.BlockSpec(memory_space=pltpu.HBM), pl.BlockSpec(memory_space=pltpu.VMEM)
        pieces = RING * RING
        out = pl.pallas_call(
            functools.partial(kernel, chunks),
            out_shape=[whole] * 3
            + [moment] * 6
            + [jax.ShapeDtypeStruct((count * pieces * nt, 8, 128), BF16), jax.ShapeDtypeStruct((count * 12 * nt, 8, 128), BF16)],
            in_specs=[hbm] * 12,
            out_specs=[vmem] * 9 + [hbm] * 2,
            scratch_shapes=[
                pltpu.VMEM((SLOTS, pieces * nt, 8, 128), BF16),
                pltpu.VMEM((EARLY_SLOTS, 8 * nt, 8, 128), BF16),
                pltpu.VMEM((SLOTS, 8 * nt, 8, 128), BF16),
                pltpu.VMEM((SLOTS, 12 * nt, 8, 128), BF16),
                pltpu.VMEM((count, 3 * nt, 8, 128), BF16),
                pltpu.SemaphoreType.DMA((count, 37)),
                pltpu.SemaphoreType.DMA((count, 3)),
                pltpu.SemaphoreType.DMA((count, 17)),
            ],
            compiler_params=pltpu.CompilerParams(collective_id=0, has_side_effects=True, vmem_limit_bytes=VMEM_LIMIT),
        )(*blocks, *moments)[:9]
        out = [pltpu.with_memory_space_constraint(o, pltpu.VMEM) for o in out]
        out = pl.pallas_call(
            put,
            out_shape=[jax.ShapeDtypeStruct(o.shape, o.dtype) for o in out],
            in_specs=[vmem] * 9,
            out_specs=[hbm] * 9,
            scratch_shapes=[pltpu.SemaphoreType.DMA((4 * layers * 9,))],
            compiler_params=pltpu.CompilerParams(vmem_limit_bytes=VMEM_LIMIT),
        )(*out)
        new = [from_tiles(o.reshape(layers, group, tiles, 8, 128), group * s[1], s[2]) for o, s in zip(out[:3], shapes, strict=True)]
        moved = [from_tiles(o.reshape(layers, 1, tiles, 8, 128), s[1], s[2]) for o, s in zip(out[3:9], shapes * 2, strict=True)]
        return (*new, *moved)

    all_of, cut = P(None, None, None), P(None, "dp", None)
    return jax.shard_map(
        step,
        mesh=mesh,
        in_specs=(P(("rep", "dp"), None, None, None),) * 3 + (all_of,) * 3 + (cut,) * 6,
        out_specs=(P("rep", None, None),) * 3 + (P("rep", "dp", None),) * 6,
        check_vma=False,
    )
```
